32 devices in a mesh: dp: 1 (over z), eo: 4 (over y), em: 4 (over x), ei: 2 (over core).
Axes of the slice: x: 4, y: 4, z: 1, core: 2. Of those that a mesh axis runs over, the one named last changes fastest.
The devices are a block of a 4x4x8 slice.
Arguments:
- x_disp: bfloat16 [32, 128, 16, 2048], P('dp', ('eo', 'em', 'ei'))
- w_gate: bfloat16 [128, 2048, 768], P(('eo', 'em', 'ei'))
- w_up: bfloat16 [128, 2048, 768], P(('eo', 'em', 'ei'))
- w_down: bfloat16 [128, 768, 2048], P(('eo', 'em', 'ei'))
- slot_idx: int32 [4096, 8], P(('dp', 'eo', 'em', 'ei'))
- expert_idx: int32 [4096, 8], P(('dp', 'eo', 'em', 'ei'))
- gate_wt: float32 [4096, 8], P(('dp', 'eo', 'em', 'ei'))
Outputs:
- output: bfloat16 [4096, 2048], P(('dp', 'eo', 'em', 'ei'))
All inputs are finite; a program needn't handle non-finite values.
Results may differ from the reference program's by a relative error of at most 0.0013.
Values are sent between devices in bfloat16 or wider.
A program may use at most 768 MiB of HBM per device.

```python
import jax
import jax.numpy as jnp
from jax import lax

D = 2048
FF = 768
EXPERTS = 128
TOP = 8
TOK_DEV = 128
GROUP = 32
SLOTS = 16
TOKENS = GROUP * TOK_DEV


def assign_slots(flat_ids):
    sort_order = jnp.argsort(flat_ids, stable=True)
    sorted_ids = flat_ids[sort_order]
    counts = jnp.bincount(flat_ids, length=EXPERTS)
    starts = jnp.cumsum(counts) - counts
    rank_sorted = jnp.arange(TOK_DEV * TOP) - starts[sorted_ids]
    slot_rank = jnp.zeros_like(rank_sorted).at[sort_order].set(rank_sorted)
    return jnp.where(slot_rank < SLOTS, slot_rank, -1).astype(jnp.int32)


def draw_routing(route_key):
    noise_key, bias_key, hot_key, shift_key = jax.random.split(route_key, 4)
    expert_ids = jnp.arange(EXPERTS, dtype=jnp.int32)
    popularity = jax.random.randint(bias_key, (EXPERTS,), 0, 48, dtype=jnp.int32)
    hot_expert = jax.random.randint(hot_key, (), 0, EXPERTS, dtype=jnp.int32)
    popularity = jnp.where(expert_ids == hot_expert, 100000, popularity)
    score_noise = jax.random.randint(noise_key, (TOKENS, EXPERTS), 0, 64, dtype=jnp.int32)
    route_score = (score_noise + popularity[None, :]) * EXPERTS + expert_ids[None, :]
    chosen = lax.top_k(route_score, TOP)[1]
    col_shift = jax.random.randint(shift_key, (TOKENS, 1), 0, TOP, dtype=jnp.int32)
    column = (jnp.arange(TOP, dtype=jnp.int32)[None, :] + col_shift) % TOP
    chosen = jnp.take_along_axis(chosen, column, axis=1).astype(jnp.int32)
    slot_idx = jax.vmap(assign_slots)(chosen.reshape(GROUP, TOK_DEV * TOP))
    return slot_idx.reshape(TOKENS, TOP), chosen


def setup_inputs(seed: int = 0, part: int = 0) -> dict:
    part_key = jax.random.fold_in(jax.random.key(seed), part)
    x_key, route_key, gate_key = jax.random.split(part_key, 3)
    wg_key, wu_key, wd_key = jax.random.split(jax.random.key(seed + 1), 3)
    x_disp = jax.random.normal(x_key, (GROUP, EXPERTS, SLOTS, D), jnp.float32).astype(jnp.bfloat16)
    w_gate = (jax.random.normal(wg_key, (EXPERTS, D, FF), jnp.float32) * D ** -0.5).astype(jnp.bfloat16)
    w_up = (jax.random.normal(wu_key, (EXPERTS, D, FF), jnp.float32) * D ** -0.5).astype(jnp.bfloat16)
    w_down = (jax.random.normal(wd_key, (EXPERTS, FF, D), jnp.float32) * (1.5 * FF ** -0.5)).astype(jnp.bfloat16)
    slot_idx, expert_idx = draw_routing(route_key)
    gate_wt = jax.nn.softmax(1.2 * jax.random.normal(gate_key, (TOKENS, TOP), jnp.float32), axis=-1)
    return {'x_disp': x_disp, 'w_gate': w_gate, 'w_up': w_up, 'w_down': w_down,
            'slot_idx': slot_idx, 'expert_idx': expert_idx, 'gate_wt': gate_wt}


def reference(x_disp, w_gate, w_up, w_down, slot_idx, expert_idx, gate_wt):
    def expert_rows(operands):
        x_rows, wg_e, wu_e, wd_e = operands
        flat_rows = x_rows.reshape(GROUP * SLOTS, D)
        gate_pre = jnp.dot(flat_rows, wg_e, preferred_element_type=jnp.float32)
        up_pre = jnp.dot(flat_rows, wu_e, preferred_element_type=jnp.float32)
        hidden = (jax.nn.silu(gate_pre) * up_pre).astype(jnp.bfloat16)
        y_flat = jnp.dot(hidden, wd_e, preferred_element_type=jnp.float32).astype(jnp.bfloat16)
        return y_flat.reshape(GROUP, SLOTS, D)

    y_rows = lax.map(expert_rows, (jnp.swapaxes(x_disp, 0, 1), w_gate, w_up, w_down))
    source = (jnp.arange(TOKENS, dtype=jnp.int32) // TOK_DEV)[:, None]
    is_live = slot_idx >= 0
    row_index = jnp.where(is_live, (expert_idx * GROUP + source) * SLOTS + slot_idx, 0)
    weight = jnp.where(is_live, gate_wt, 0.0)
    picked = jnp.take(y_rows.reshape(EXPERTS * GROUP * SLOTS, D), row_index, axis=0)
    combined = jnp.sum(weight[:, :, None] * picked.astype(jnp.float32), axis=1)
    return combined.astype(jnp.bfloat16)
```

```python
import functools

import jax
import jax.numpy as jnp
from jax import lax
from jax.experimental import pallas as pl
from jax.experimental.pallas import tpu as pltpu
from jax.sharding import PartitionSpec as P

GROUP_AXES = ('eo', 'em', 'ei')
MESH_ID = pl.DeviceIdType.MESH
BF16_MAX = 3.3895313892515355e38


def _split3(w):
    hi = w.astype(jnp.bfloat16)
    rest = w - hi.astype(jnp.float32)
    mid = rest.astype(jnp.bfloat16)
    low = (rest - mid.astype(jnp.float32)).astype(jnp.bfloat16)
    return jnp.concatenate([hi, mid, low], axis=0)


def _body(sizes, x_hbm, wg_hbm, wu_hbm, wd_hbm, slot_ref, exp_ref, gate_ref, o_ref,
          xbuf, wgbuf, wubuf, wdbuf, hbuf, ybuf, rbuf, wbuf, pbuf, far, near,
          rslot, rexp, rgate,
          in_sem, route_send, route_recv, loc_sem, s1_send, s1_recv, s2_send, s2_recv):
    YN, XN, CN, EN, SN, DN, FN, TN = sizes
    RING = YN
    HALF = DN // 2
    ROWS = YN * XN * CN * SN
    KROW = XN * CN * EN * SN
    TF = min(256, FN)
    TD = min(256, HALF)
    y = lax.axis_index('eo')
    x = lax.axis_index('em')
    c = lax.axis_index('ei')

    def at(dy, dx, dc):
        return {'eo': lax.rem(y + dy + YN, YN), 'em': lax.rem(x + dx + XN, XN), 'ei': lax.rem(c + dc + CN, CN)}

    def along(h, d, dc=0):
        return at(d, 0, dc) if h else at(0, d, dc)

    def loads(e):
        b = e % 2
        return (pltpu.make_async_copy(x_hbm.at[:, e], xbuf.at[b], in_sem.at[b, 0]),
                pltpu.make_async_copy(wg_hbm.at[e], wgbuf.at[b], in_sem.at[b, 1]),
                pltpu.make_async_copy(wu_hbm.at[e], wubuf.at[b], in_sem.at[b, 2]),
                pltpu.make_async_copy(wd_hbm.at[e], wdbuf.at[b], in_sem.at[b, 3]))

    for cp in loads(0):
        cp.start()

    peers = [at(0, d, dc) for d in range(XN) for dc in range(CN) if (d, dc) != (0, 0)]
    peers += [at(d, 0, dc) for d in range(1, YN) for dc in range(CN)]
    barrier = pltpu.get_barrier_semaphore()
    for p in peers:
        pl.semaphore_signal(barrier, inc=1, device_id=p, device_id_type=MESH_ID)
    pl.semaphore_wait(barrier, len(peers))

    def routes(h, d):
        dev = along(1 - h, d)
        return [pltpu.make_async_remote_copy(src_ref=src, dst_ref=dst.at[h, d], send_sem=route_send.at[h, d, i],
                                             recv_sem=route_recv.at[h, d, i], device_id=dev, device_id_type=MESH_ID)
                for i, (src, dst) in enumerate(((slot_ref, rslot), (exp_ref, rexp), (gate_ref, rgate)))]
    for h in range(2):
        for d in range(1, RING):
            for cp in routes(h, d):
                cp.start()

    def s1(h, e, d, dc):
        tgt = along(h, d, dc)
        ctgt = tgt['ei']
        if h == 0:
            src = ybuf.at[e, :, tgt['em'], ctgt, :, pl.ds(0, HALF)]
            dst = rbuf.at[0, :, x, c, e]
        else:
            src = ybuf.at[e, tgt['eo'], :, ctgt, :, pl.ds(HALF, HALF)]
            dst = rbuf.at[1, :, y, c, e]
        if (d, dc) == (0, 0):
            return pltpu.make_async_copy(src, dst, loc_sem.at[h, e])
        return pltpu.make_async_remote_copy(src_ref=src, dst_ref=dst, send_sem=s1_send.at[h, e, d, dc],
                                            recv_sem=s1_recv.at[h, e, d, dc], device_id=tgt, device_id_type=MESH_ID)
    order = [(2, 0), (2, 1), (1, 0), (3, 0), (1, 1), (3, 1), (0, 1), (0, 0)]

    for e in range(EN):
        b = e % 2
        lx, lg, lu, ld = loads(e)
        lx.wait()
        lg.wait()
        lu.wait()
        if e + 1 < EN:
            for cp in loads(e + 1):
                cp.start()

        def gate_up(n, carry):
            cols = pl.ds(pl.multiple_of(n * TF, TF), TF)
            xv = xbuf[b].reshape(ROWS, DN)
            g = jnp.dot(xv, wgbuf[b, :, cols], preferred_element_type=jnp.float32)
            u = jnp.dot(xv, wubuf[b, :, cols], preferred_element_type=jnp.float32)
            hbuf[:, cols] = (jax.nn.silu(g) * u).astype(jnp.bfloat16)
            return carry
        lax.fori_loop(0, FN // TF, gate_up, 0)
        ld.wait()

        def down(n, carry):
            cols = pl.ds(pl.multiple_of(n * TD, TD), TD)
            v = jnp.dot(hbuf[...], wdbuf[b, :, cols], preferred_element_type=jnp.float32)
            v = jnp.where(jnp.abs(v) < BF16_MAX, v, 0.0)
            ybuf[e, :, :, :, :, cols] = v.astype(jnp.bfloat16).reshape(YN, XN, CN, SN, TD)
            return carry
        for h in range(2):
            lax.fori_loop(h * (HALF // TD), (h + 1) * (HALF // TD), down, 0)
            for d, dc in order:
                s1(h, e, d, dc).start()

    def build(h, d):
        if d == 0:
            sl, ex, ga = slot_ref[...], exp_ref[...], gate_ref[...]
        else:
            sl, ex, ga = rslot[h, d], rexp[h, d], rgate[h, d]
        code = jnp.where(sl >= 0, ex * SN + sl, -1)
        if h == 0:
            col = jnp.where(code >= 0, code - y * KROW, -1)
        else:
            blk = CN * EN * SN
            ye = code // KROW
            rem = code - ye * KROW - x * blk
            col = jnp.where((code >= 0) & (rem >= 0) & (rem < blk), ye * blk + rem, -1)
        col = jnp.transpose(col.astype(jnp.float32)).astype(jnp.int32)
        ga = jnp.transpose(ga)
        lanes = lax.broadcasted_iota(jnp.int32, (TN, KROW), 1)
        w = jnp.zeros((TN, KROW), jnp.float32)
        for j in range(col.shape[1]):
            w = w + jnp.where(lanes == col[:, j:j + 1], ga[:, j:j + 1], 0.0)
        wbuf[h, d] = _split3(w)
    for h in range(2):
        for d in range(RING):
            if d:
                for cp in routes(h, d):
                    cp.wait_recv()
            build(h, d)

    for h in range(2):
        for e in range(EN):
            for d, dc in order:
                if (d, dc) == (0, 0):
                    s1(h, e, 0, 0).wait()
                else:
                    s1(h, e, d, dc).wait_recv()

    def combine(h, d):
        pos = lax.rem((x if h else y) - d + RING, RING)

        def step(n, carry):
            cols = pl.ds(pl.multiple_of(n * TD, TD), TD)
            rows = rbuf[h, pos, :, :, :, :, cols].reshape(KROW, TD)
            v = jnp.dot(wbuf[h, d], rows, preferred_element_type=jnp.float32)
            pbuf[h, d, :, cols] = v[0:TN] + (v[TN:2 * TN] + v[2 * TN:3 * TN])
            return carry
        lax.fori_loop(0, HALF // TD, step, 0)

    TH = TN // 2

    def s2_far(h, up):
        rows = pl.ds(0, TH) if up else pl.ds(TH, TH)
        i = 0 if up else 1
        return pltpu.make_async_remote_copy(src_ref=pbuf.at[h, 2, rows], dst_ref=far.at[h, i], send_sem=s2_send.at[h, i],
                                            recv_sem=s2_recv.at[h, i], device_id=along(1 - h, 1 if up else -1),
                                            device_id_type=MESH_ID)

    def s2_near(h, up):
        d = RING - 1 if up else 1
        i = 0 if up else 1
        return pltpu.make_async_remote_copy(src_ref=pbuf.at[h, d], dst_ref=near.at[h, i], send_sem=s2_send.at[h, 2 + i],
                                            recv_sem=s2_recv.at[h, 2 + i], device_id=along(1 - h, 1 if up else -1),
                                            device_id_type=MESH_ID)

    combine(0, 2)
    combine(1, 2)
    for h in range(2):
        s2_far(h, True).start()
        s2_far(h, False).start()
    for h in range(2):
        combine(h, RING - 1)
        combine(h, 1)
    for h in range(2):
        s2_far(h, True).wait_recv()
        pbuf[h, RING - 1, 0:TH] += far[h, 0]
        s2_far(h, False).wait_recv()
        pbuf[h, 1, TH:TN] += far[h, 1]
        s2_near(h, True).start()
        s2_near(h, False).start()
    for h in range(2):
        combine(h, 0)
    for h in range(2):
        s2_near(h, True).wait_recv()
        s2_near(h, False).wait_recv()
        o_ref[:, h * HALF:(h + 1) * HALF] = (pbuf[h, 0] + near[h, 0] + near[h, 1]).astype(o_ref.dtype)

    for h in range(2):
        for d in range(1, RING):
            for cp in routes(h, d):
                cp.wait_send()
        for e in range(EN):
            for d, dc in order:
                if (d, dc) != (0, 0):
                    s1(h, e, d, dc).wait_send()
        for up in (True, False):
            s2_far(h, up).wait_send()
            s2_near(h, up).wait_send()


def solution(mesh):
    token_spec = P(('dp',) + GROUP_AXES, None)
    weight_spec = P(GROUP_AXES, None, None)
    rows_spec = P('dp', GROUP_AXES, None, None)
    YN, XN, CN = (mesh.shape[a] for a in GROUP_AXES)

    def local_part(x_local, w_gate, w_up, w_down, slot_idx, expert_idx, gate_wt):
        _, EN, SN, DN = x_local.shape
        FN = w_gate.shape[2]
        TN, TOP = slot_idx.shape
        HALF = DN // 2
        RING = YN
        KROW = XN * CN * EN * SN
        sizes = (YN, XN, CN, EN, SN, DN, FN, TN)
        bf, f32, i32 = jnp.bfloat16, jnp.float32, jnp.int32
        vm, dma = pltpu.VMEM, pltpu.SemaphoreType.DMA
        any_spec = pl.BlockSpec(memory_space=pltpu.HBM)
        vmem_spec = pl.BlockSpec(memory_space=pltpu.VMEM)
        return pl.pallas_call(
            functools.partial(_body, sizes),
            out_shape=jax.ShapeDtypeStruct((TN, DN), bf),
            in_specs=[any_spec] * 4 + [vmem_spec] * 3,
            out_specs=vmem_spec,
            scratch_shapes=[
                vm((2, YN * XN * CN, SN, DN), bf), vm((2, DN, FN), bf), vm((2, DN, FN), bf), vm((2, FN, DN), bf),
                vm((YN * XN * CN * SN, FN), bf),
                vm((EN, YN, XN, CN, SN, DN), bf),
                vm((2, RING, RING, CN, EN, SN, HALF), bf),
                vm((2, RING, 3 * TN, KROW), bf),
                vm((2, RING, TN, HALF), f32),
                vm((2, 2, TN // 2, HALF), f32),
                vm((2, 2, TN, HALF), f32),
                vm((2, RING, TOP, TN), i32), vm((2, RING, TOP, TN), i32), vm((2, RING, TOP, TN), f32),
                dma((2, 4)), dma((2, RING, 3)), dma((2, RING, 3)), dma((2, EN)),
                dma((2, EN, RING, CN)), dma((2, EN, RING, CN)), dma((2, 4)), dma((2, 4)),
            ],
            compiler_params=pltpu.CompilerParams(collective_id=0, has_side_effects=True,
                                                 vmem_limit_bytes=62 * 2 ** 20),
        )(x_local, w_gate, w_up, w_down, slot_idx.T, expert_idx.T, gate_wt.T)

    return jax.shard_map(local_part, mesh=mesh,
                         in_specs=(rows_spec, weight_spec, weight_spec, weight_spec, token_spec, token_spec, token_spec),
                         out_specs=token_spec, check_vma=False)
```

```python
import functools

import jax
import jax.numpy as jnp
from jax import lax
from jax.experimental import pallas as pl
from jax.experimental.pallas import tpu as pltpu
from jax.sharding import PartitionSpec as P

GROUP_AXES = ('eo', 'em', 'ei')
MESH_ID = pl.DeviceIdType.MESH
BF16_MAX = 3.3895313892515355e38


def _split3(w):
    hi = w.astype(jnp.bfloat16)
    rest = w - hi.astype(jnp.float32)
    mid = rest.astype(jnp.bfloat16)
    low = (rest - mid.astype(jnp.float32)).astype(jnp.bfloat16)
    return jnp.concatenate([hi, mid, low], axis=0)


def _body(sizes, x_hbm, wg_hbm, wu_hbm, wd_hbm, slot_ref, exp_ref, gate_ref, o_ref,
          xbuf, wgbuf, wubuf, wdbuf, hbuf, ya, yb, rbuf, wbuf, pbuf, far, near,
          rslot, rexp, rgate,
          x_sem, wg_sem, wu_sem, wd_sem, route_send, route_recv, loc_sem, s1_send, s1_recv, s2_send, s2_recv):
    YN, XN, CN, EN, SN, DN, FN, TN = sizes
    RING = YN
    HALF = DN // 2
    QROWS = XN * CN * SN
    KROW = XN * CN * EN * SN
    TF = min(256, FN)
    TD = min(256, HALF)
    TH = TN // 2
    UP, FAR, DOWN, OWN = 0, 1, 2, 3
    y = lax.axis_index('eo')
    x = lax.axis_index('em')
    c = lax.axis_index('ei')

    def at(dy, dx, dc):
        return {'eo': lax.rem(y + dy + YN, YN), 'em': lax.rem(x + dx + XN, XN), 'ei': lax.rem(c + dc + CN, CN)}

    def along(h, d, dc=0):
        return at(d, 0, dc) if h else at(0, d, dc)

    def load_x(e, q):
        ys = lax.rem(y + q + 1, YN)
        return pltpu.make_async_copy(x_hbm.at[pl.ds(ys * XN * CN, XN * CN), e],
                                     xbuf.at[e % 2, pl.ds(q * XN * CN, XN * CN)], x_sem.at[e % 2, q])

    def load_tile(e, src, dst, sem, n):
        cols = pl.ds(pl.multiple_of(n * TF, TF), TF)
        return pltpu.make_async_copy(src.at[e, :, cols], dst.at[e % 2, :, cols], sem.at[e % 2, n])

    def load_down(e):
        return pltpu.make_async_copy(wd_hbm.at[e], wdbuf.at[e % 2], wd_sem.at[e % 2])

    NT = FN // TF

    def start_loads(e):
        for q in range(2):
            load_x(e, q).start()
        for n in range(NT):
            load_tile(e, wg_hbm, wgbuf, wg_sem, n).start()
            load_tile(e, wu_hbm, wubuf, wu_sem, n).start()
        for q in range(2, RING):
            load_x(e, q).start()
        load_down(e).start()

    start_loads(0)

    peers = [at(0, d, dc) for d in range(XN) for dc in range(CN) if (d, dc) != (0, 0)]
    peers += [at(d, 0, dc) for d in range(1, YN) for dc in range(CN)]
    barrier = pltpu.get_barrier_semaphore()
    for p in peers:
        pl.semaphore_signal(barrier, inc=1, device_id=p, device_id_type=MESH_ID)

    def routes(h, q):
        dev = along(1 - h, -(q + 1))
        return [pltpu.make_async_remote_copy(src_ref=src, dst_ref=dst.at[h, q], send_sem=route_send.at[h, q, i],
                                             recv_sem=route_recv.at[h, q, i], device_id=dev, device_id_type=MESH_ID)
                for i, (src, dst) in enumerate(((slot_ref, rslot), (exp_ref, rexp), (gate_ref, rgate)))]

    messages = {}

    def s1(name, h, es, qs, d, dc):
        i = messages.setdefault((name, h), len(messages))
        tgt = along(h, d, dc)
        if es[1] - es[0] == 1:
            esl, qsl = es[0], pl.ds(qs[0], qs[1] - qs[0])
        else:
            esl, qsl = pl.ds(es[0], es[1] - es[0]), qs[0]
        if h == 0:
            src = ya.at[esl, qsl, tgt['em'], tgt['ei']]
            dst = rbuf.at[0, qsl, x, c, esl]
        else:
            src = yb.at[esl, qsl, (d + RING - 1) % RING, tgt['ei']]
            dst = rbuf.at[1, qsl, y, c, esl]
        if (d, dc) == (0, 0):
            return pltpu.make_async_copy(src, dst, loc_sem.at[i])
        return pltpu.make_async_remote_copy(src_ref=src, dst_ref=dst, send_sem=s1_send.at[i, d, dc],
                                            recv_sem=s1_recv.at[i, d, dc], device_id=tgt, device_id_type=MESH_ID)

    ORDER = [(2, 0), (1, 0), (3, 0), (2, 1), (1, 1), (3, 1), (0, 1), (0, 0)]
    sent = []

    def send(name, h, es, qs, ds=(0, 1, 2, 3)):
        if (name, h, es, qs) not in sent:
            sent.append((name, h, es, qs))
        for d, dc in ORDER:
            if d in ds:
                s1(name, h, es, qs, d, dc).start()

    def arrived(name, h, es, qs):
        for d, dc in ORDER:
            cp = s1(name, h, es, qs, d, dc)
            cp.wait() if (d, dc) == (0, 0) else cp.wait_recv()

    def gate_up(e, q0, q1, first):
        b = e % 2
        rows = (q1 - q0) * QROWS

        def step(n, carry):
            cols = pl.ds(pl.multiple_of(n * TF, TF), TF)
            if first:
                load_tile(e, wg_hbm, wgbuf, wg_sem, n).wait()
                load_tile(e, wu_hbm, wubuf, wu_sem, n).wait()
            xv = xbuf[b, q0 * XN * CN:q1 * XN * CN].reshape(rows, DN)
            g = jnp.dot(xv, wgbuf[b, :, cols], preferred_element_type=jnp.float32)
            u = jnp.dot(xv, wubuf[b, :, cols], preferred_element_type=jnp.float32)
            hbuf[q0 * QROWS:q1 * QROWS, cols] = (jax.nn.silu(g) * u).astype(jnp.bfloat16)
            return carry
        lax.fori_loop(0, NT, step, 0)

    def down(e, q0, q1, h):
        b = e % 2

        def step(n, carry):
            wcols = pl.ds(pl.multiple_of(h * HALF + n * TD, TD), TD)
            cols = pl.ds(pl.multiple_of(n * TD, TD), TD)
            v = jnp.dot(hbuf[q0 * QROWS:q1 * QROWS], wdbuf[b, :, wcols], preferred_element_type=jnp.float32)
            v = jnp.where(jnp.abs(v) < BF16_MAX, v, 0.0)
            v = v.astype(jnp.bfloat16).reshape(q1 - q0, XN, CN, SN, TD)
            if h == 0:
                ya[e, q0:q1, :, :, :, cols] = v
            else:
                for xs in range(XN):
                    yb[e, lax.rem(xs - x - 1 + 2 * XN, XN), q0:q1, :, :, cols] = v[:, xs]
            return carry
        lax.fori_loop(0, HALF // TD, step, 0)

    for q in range(2):
        load_x(0, q).wait()
    gate_up(0, 0, 2, True)
    load_down(0).wait()
    down(0, 0, 2, 0)
    pl.semaphore_wait(barrier, len(peers))
    send('a', 0, (0, 1), (0, 2))
    down(0, 0, 2, 1)
    send('a', 1, (0, 1), (0, 4), (1, 2))
    for h in range(2):
        for q in range(RING - 1):
            for cp in routes(h, q):
                cp.start()
    for q in range(2, RING):
        load_x(0, q).wait()
    start_loads(1)
    gate_up(0, 2, 4, False)
    down(0, 2, 4, 0)
    send('b', 0, (0, 1), (2, 4))
    down(0, 2, 4, 1)
    send('a', 1, (0, 1), (0, 4), (3, 0))

    HELD = EN - 2
    for e in range(1, EN):
        for q in range(RING):
            load_x(e, q).wait()
        if e + 1 < EN:
            start_loads(e + 1)
        gate_up(e, 0, RING, True)
        load_down(e).wait()
        for h in range(2):
            down(e, 0, RING, h)
            send(e, h, (e, e + 1), (0, RING if e < HELD else RING - 1))
    for h in range(2):
        send('own', h, (HELD, EN), (OWN, OWN + 1))

    def build(h, q):
        if q == OWN:
            sl, ex, ga = slot_ref[...], exp_ref[...], gate_ref[...]
        else:
            sl, ex, ga = rslot[h, q], rexp[h, q], rgate[h, q]
        code = jnp.where(sl >= 0, ex * SN + sl, -1)
        if h == 0:
            col = jnp.where(code >= 0, code - y * KROW, -1)
        else:
            blk = CN * EN * SN
            ye = code // KROW
            rem = code - ye * KROW - x * blk
            col = jnp.where((code >= 0) & (rem >= 0) & (rem < blk), ye * blk + rem, -1)
        col = jnp.transpose(col.astype(jnp.float32)).astype(jnp.int32)
        ga = jnp.transpose(ga)
        lanes = lax.broadcasted_iota(jnp.int32, (TN, KROW), 1)
        w = jnp.zeros((TN, KROW), jnp.float32)
        for j in range(col.shape[1]):
            w = jnp.where(lanes == col[:, j:j + 1], ga[:, j:j + 1], w)
        wbuf[h, q] = _split3(w)

    for h in range(2):
        for q in range(RING):
            if q != OWN:
                for cp in routes(h, q):
                    cp.wait_recv()
            build(h, q)

    def combine(h, q):
        def step(n, carry):
            cols = pl.ds(pl.multiple_of(n * TD, TD), TD)
            rows = rbuf[h, q, :, :, :, :, cols].reshape(KROW, TD)
            v = jnp.dot(wbuf[h, q], rows, preferred_element_type=jnp.float32)
            pbuf[h, q, :, cols] = v[0:TN] + (v[TN:2 * TN] + v[2 * TN:3 * TN])
            return carry
        lax.fori_loop(0, HALF // TD, step, 0)

    def s2(h, what, up):
        i = 0 if up else 1
        low, high = pl.ds(0, TH), pl.ds(TH, TH)
        if what == 0:
            src, dst = pbuf.at[h, FAR, low if up else high], far.at[h, i]
        else:
            rows = (high if up else low) if what == 1 else (low if up else high)
            src, dst = pbuf.at[h, UP if up else DOWN, rows], near.at[h, i, rows]
        return pltpu.make_async_remote_copy(src_ref=src, dst_ref=dst, send_sem=s2_send.at[h, what, i],
                                            recv_sem=s2_recv.at[h, what, i], device_id=along(1 - h, 1 if up else -1),
                                            device_id_type=MESH_ID)

    for h in range(2):
        for key in sent:
            if key[1] == h and key[0] != 'own':
                arrived(*key)
        combine(h, FAR)
    for h in range(2):
        s2(h, 0, True).start()
        s2(h, 0, False).start()
    for h in range(2):
        combine(h, UP)
        combine(h, DOWN)
    for h in range(2):
        s2(h, 1, True).start()
        s2(h, 1, False).start()
    for h in range(2):
        s2(h, 0, True).wait_recv()
        pbuf[h, UP, 0:TH] += far[h, 0]
        s2(h, 0, False).wait_recv()
        pbuf[h, DOWN, TH:TN] += far[h, 1]
        s2(h, 2, True).start()
        s2(h, 2, False).start()
    for h in range(2):
        for key in sent:
            if key[1] == h and key[0] == 'own':
                arrived(*key)
        combine(h, OWN)
    for h in range(2):
        s2(h, 1, True).wait_recv()
        pbuf[h, OWN, TH:TN] += near[h, 0, TH:TN]
        s2(h, 1, False).wait_recv()
        pbuf[h, OWN, 0:TH] += near[h, 1, 0:TH]
    for h in range(2):
        s2(h, 2, True).wait_recv()
        o_ref[0:TH, h * HALF:(h + 1) * HALF] = (pbuf[h, OWN, 0:TH] + near[h, 0, 0:TH]).astype(o_ref.dtype)
        s2(h, 2, False).wait_recv()
        o_ref[TH:TN, h * HALF:(h + 1) * HALF] = (pbuf[h, OWN, TH:TN] + near[h, 1, TH:TN]).astype(o_ref.dtype)

    for h in range(2):
        for q in range(RING - 1):
            for cp in routes(h, q):
                cp.wait_send()
        for what in range(3):
            for up in (True, False):
                s2(h, what, up).wait_send()
    for key in sent:
        for d, dc in ORDER:
            if (d, dc) != (0, 0):
                s1(*key, d, dc).wait_send()


def solution(mesh):
    token_spec = P(('dp',) + GROUP_AXES, None)
    weight_spec = P(GROUP_AXES, None, None)
    rows_spec = P('dp', GROUP_AXES, None, None)
    YN, XN, CN = (mesh.shape[a] for a in GROUP_AXES)

    def local_part(x_local, w_gate, w_up, w_down, slot_idx, expert_idx, gate_wt):
        _, EN, SN, DN = x_local.shape
        FN = w_gate.shape[2]
        TN, TOP = slot_idx.shape
        HALF = DN // 2
        RING = YN
        KROW = XN * CN * EN * SN
        sizes = (YN, XN, CN, EN, SN, DN, FN, TN)
        bf, f32, i32 = jnp.bfloat16, jnp.float32, jnp.int32
        vm, dma = pltpu.VMEM, pltpu.SemaphoreType.DMA
        any_spec = pl.BlockSpec(memory_space=pltpu.HBM)
        vmem_spec = pl.BlockSpec(memory_space=pltpu.VMEM)
        return pl.pallas_call(
            functools.partial(_body, sizes),
            out_shape=vm((TN, DN), bf),
            in_specs=[any_spec] * 4 + [vmem_spec] * 3,
            out_specs=vmem_spec,
            scratch_shapes=[
                vm((2, YN * XN * CN, SN, DN), bf), vm((2, DN, FN), bf), vm((2, DN, FN), bf), vm((2, FN, DN), bf),
                vm((YN * XN * CN * SN, FN), bf),
                vm((EN, YN, XN, CN, SN, HALF), bf), vm((EN, XN, YN, CN, SN, HALF), bf),
                vm((2, RING, RING, CN, EN, SN, HALF), bf),
                vm((2, RING, 3 * TN, KROW), bf),
                vm((2, RING, TN, HALF), f32),
                vm((2, 2, TN // 2, HALF), f32),
                vm((2, 2, TN, HALF), f32),
                vm((2, RING, TOP, TN), i32), vm((2, RING, TOP, TN), i32), vm((2, RING, TOP, TN), f32),
                dma((2, RING)), dma((2, FN // min(256, FN))), dma((2, FN // min(256, FN))), dma((2,)),
                dma((2, RING, 3)), dma((2, RING, 3)), dma((2 * EN + 4,)),
                dma((2 * EN + 4, RING, CN)), dma((2 * EN + 4, RING, CN)), dma((2, 3, 2)), dma((2, 3, 2)),
            ],
            compiler_params=pltpu.CompilerParams(collective_id=0, has_side_effects=True,
                                                 vmem_limit_bytes=62 * 2 ** 20),
        )(x_local, w_gate, w_up, w_down, slot_idx.T, expert_idx.T, gate_wt.T)

    return jax.shard_map(local_part, mesh=mesh,
                         in_specs=(rows_spec, weight_spec, weight_spec, weight_spec, token_spec, token_spec, token_spec),
                         out_specs=token_spec, check_vma=False)
```

```python
import functools

import jax
import jax.numpy as jnp
from jax import lax
from jax.experimental import pallas as pl
from jax.experimental.pallas import tpu as pltpu
from jax.sharding import PartitionSpec as P

GROUP_AXES = ('eo', 'em', 'ei')
MESH_ID = pl.DeviceIdType.MESH
BF16_MAX = 3.3895313892515355e38


def _split3(w):
    hi = w.astype(jnp.bfloat16)
    rest = w - hi.astype(jnp.float32)
    mid = rest.astype(jnp.bfloat16)
    low = (rest - mid.astype(jnp.float32)).astype(jnp.bfloat16)
    return jnp.concatenate([hi, mid, low], axis=0)


def _body(sizes, x_hbm, wg_hbm, wu_hbm, wd_hbm, slot_ref, exp_ref, gate_ref, o_ref,
          xbuf, wgbuf, wubuf, wdbuf, hbuf, ya, yb, rbuf, wbuf, pbuf, far, near,
          rslot, rexp, rgate,
          x_sem, wg_sem, wu_sem, wd_sem, route_send, route_recv, loc_sem, s1_send, s1_recv, s2_send, s2_recv):
    YN, XN, CN, EN, SN, DN, FN, TN = sizes
    RING = YN
    HALF = DN // 2
    QROWS = XN * CN * SN
    KROW = XN * CN * EN * SN
    TF = min(256, FN)
    TD = min(1024, HALF)
    TC = min(256, HALF)
    TH = TN // 2
    UP, FAR, DOWN, OWN = 0, 1, 2, 3
    y = lax.axis_index('eo')
    x = lax.axis_index('em')
    c = lax.axis_index('ei')

    def at(dy, dx, dc):
        return {'eo': lax.rem(y + dy + YN, YN), 'em': lax.rem(x + dx + XN, XN), 'ei': lax.rem(c + dc + CN, CN)}

    def along(h, d, dc=0):
        return at(d, 0, dc) if h else at(0, d, dc)

    def load_x(e, q):
        ys = lax.rem(y + q + 1, YN)
        return pltpu.make_async_copy(x_hbm.at[pl.ds(ys * XN * CN, XN * CN), e],
                                     xbuf.at[e % 2, pl.ds(q * XN * CN, XN * CN)], x_sem.at[e % 2, q])

    def load_tile(e, src, dst, sem, n):
        cols = pl.ds(pl.multiple_of(n * TF, TF), TF)
        return pltpu.make_async_copy(src.at[e, :, cols], dst.at[e % 2, :, cols], sem.at[e % 2, n])

    def load_down(e):
        return pltpu.make_async_copy(wd_hbm.at[e], wdbuf.at[e % 2], wd_sem.at[e % 2])

    NT = FN // TF

    def start_loads(e):
        for q in range(2):
            load_x(e, q).start()
        for n in range(NT):
            load_tile(e, wg_hbm, wgbuf, wg_sem, n).start()
            load_tile(e, wu_hbm, wubuf, wu_sem, n).start()
        for q in range(2, RING):
            load_x(e, q).start()
        load_down(e).start()

    start_loads(0)

    peers = [at(0, d, dc) for d in range(XN) for dc in range(CN) if (d, dc) != (0, 0)]
    peers += [at(d, 0, dc) for d in range(1, YN) for dc in range(CN)]
    barrier = pltpu.get_barrier_semaphore()
    for p in peers:
        pl.semaphore_signal(barrier, inc=1, device_id=p, device_id_type=MESH_ID)

    def routes(h, q):
        dev = along(1 - h, -(q + 1))
        return [pltpu.make_async_remote_copy(src_ref=src, dst_ref=dst.at[h, q], send_sem=route_send.at[h, q, i],
                                             recv_sem=route_recv.at[h, q, i], device_id=dev, device_id_type=MESH_ID)
                for i, (src, dst) in enumerate(((slot_ref, rslot), (exp_ref, rexp), (gate_ref, rgate)))]

    messages = {}

    def s1(name, h, es, qs, d, dc):
        i = messages.setdefault((name, h), len(messages))
        tgt = along(h, d, dc)
        if es[1] - es[0] == 1:
            esl, qsl = es[0], pl.ds(qs[0], qs[1] - qs[0])
        else:
            esl, qsl = pl.ds(es[0], es[1] - es[0]), qs[0]
        if h == 0:
            src = ya.at[esl, qsl, tgt['em'], tgt['ei']]
            dst = rbuf.at[0, qsl, x, c, esl]
        else:
            src = yb.at[esl, qsl, (d + RING - 1) % RING, tgt['ei']]
            dst = rbuf.at[1, qsl, y, c, esl]
        if (d, dc) == (0, 0):
            return pltpu.make_async_copy(src, dst, loc_sem.at[i])
        return pltpu.make_async_remote_copy(src_ref=src, dst_ref=dst, send_sem=s1_send.at[i, d, dc],
                                            recv_sem=s1_recv.at[i, d, dc], device_id=tgt, device_id_type=MESH_ID)

    ORDER = [(2, 0), (1, 0), (3, 0), (2, 1), (1, 1), (3, 1), (0, 1), (0, 0)]
    sent = []

    def send(name, h, es, qs, ds=(0, 1, 2, 3)):
        if (name, h, es, qs) not in sent:
            sent.append((name, h, es, qs))
        for d, dc in ORDER:
            if d in ds:
                s1(name, h, es, qs, d, dc).start()

    def arrived(name, h, es, qs):
        for d, dc in ORDER:
            cp = s1(name, h, es, qs, d, dc)
            cp.wait() if (d, dc) == (0, 0) else cp.wait_recv()

    def gate_up(e, q0, q1, tf, waits):
        b = e % 2
        rows = (q1 - q0) * QROWS
        if waits and tf != TF:
            for n in range(NT):
                load_tile(e, wg_hbm, wgbuf, wg_sem, n).wait()
                load_tile(e, wu_hbm, wubuf, wu_sem, n).wait()

        def step(n, carry):
            cols = pl.ds(pl.multiple_of(n * tf, tf), tf)
            if waits and tf == TF:
                load_tile(e, wg_hbm, wgbuf, wg_sem, n).wait()
                load_tile(e, wu_hbm, wubuf, wu_sem, n).wait()
            xv = xbuf[b, q0 * XN * CN:q1 * XN * CN].reshape(rows, DN)
            g = jnp.dot(xv, wgbuf[b, :, cols], preferred_element_type=jnp.float32)
            u = jnp.dot(xv, wubuf[b, :, cols], preferred_element_type=jnp.float32)
            hbuf[q0 * QROWS:q1 * QROWS, cols] = (jax.nn.silu(g) * u).astype(jnp.bfloat16)
            return carry
        lax.fori_loop(0, FN // tf, step, 0)

    def down(e, q0, q1, h):
        b = e % 2

        def step(n, carry):
            wcols = pl.ds(pl.multiple_of(h * HALF + n * TD, TD), TD)
            cols = pl.ds(pl.multiple_of(n * TD, TD), TD)
            v = jnp.dot(hbuf[q0 * QROWS:q1 * QROWS], wdbuf[b, :, wcols], preferred_element_type=jnp.float32)
            v = jnp.where(jnp.abs(v) < BF16_MAX, v, 0.0)
            v = v.astype(jnp.bfloat16).reshape(q1 - q0, XN, CN, SN, TD)
            if h == 0:
                ya[e, q0:q1, :, :, :, cols] = v
            else:
                for xs in range(XN):
                    yb[e, lax.rem(xs - x - 1 + 2 * XN, XN), q0:q1, :, :, cols] = v[:, xs]
            return carry
        lax.fori_loop(0, HALF // TD, step, 0)

    for q in range(2):
        load_x(0, q).wait()
    gate_up(0, 0, 2, TF, True)
    load_down(0).wait()
    down(0, 0, 2, 0)
    pl.semaphore_wait(barrier, len(peers))
    send('a', 0, (0, 1), (0, 2))
    down(0, 0, 2, 1)
    send('a', 1, (0, 1), (0, 4), (1, 2))
    for h in range(2):
        for q in range(RING - 1):
            for cp in routes(h, q):
                cp.start()
    for q in range(2, RING):
        load_x(0, q).wait()
    start_loads(1)
    gate_up(0, 2, 4, FN, False)
    down(0, 2, 4, 0)
    send('b', 0, (0, 1), (2, 4))
    down(0, 2, 4, 1)
    send('a', 1, (0, 1), (0, 4), (3, 0))

    HELD = EN - 2
    for e in range(1, EN):
        for q in range(RING):
            load_x(e, q).wait()
        if e + 1 < EN:
            start_loads(e + 1)
        gate_up(e, 0, RING, FN, True)
        load_down(e).wait()
        for h in range(2):
            down(e, 0, RING, h)
            send(e, h, (e, e + 1), (0, RING if e < HELD else RING - 1))
    for h in range(2):
        send('own', h, (HELD, EN), (OWN, OWN + 1))

    def build(h, q):
        if q == OWN:
            sl, ex, ga = slot_ref[...], exp_ref[...], gate_ref[...]
        else:
            sl, ex, ga = rslot[h, q], rexp[h, q], rgate[h, q]
        code = jnp.where(sl >= 0, ex * SN + sl, -1)
        if h == 0:
            col = jnp.where(code >= 0, code - y * KROW, -1)
        else:
            blk = CN * EN * SN
            ye = code // KROW
            rem = code - ye * KROW - x * blk
            col = jnp.where((code >= 0) & (rem >= 0) & (rem < blk), ye * blk + rem, -1)
        col = jnp.transpose(col.astype(jnp.float32)).astype(jnp.int32)
        ga = jnp.transpose(ga)
        lanes = lax.broadcasted_iota(jnp.int32, (TN, KROW), 1)
        w = jnp.zeros((TN, KROW), jnp.float32)
        for j in range(col.shape[1]):
            w = jnp.where(lanes == col[:, j:j + 1], ga[:, j:j + 1], w)
        wbuf[h, q] = _split3(w)

    for h in range(2):
        for q in range(RING):
            if q != OWN:
                for cp in routes(h, q):
                    cp.wait_recv()
            build(h, q)

    def combine(h, q):
        def step(n, carry):
            cols = pl.ds(pl.multiple_of(n * TC, TC), TC)
            rows = rbuf[h, q, :, :, :, :, cols].reshape(KROW, TC)
            v = jnp.dot(wbuf[h, q], rows, preferred_element_type=jnp.float32)
            pbuf[h, q, :, cols] = v[0:TN] + (v[TN:2 * TN] + v[2 * TN:3 * TN])
            return carry
        lax.fori_loop(0, HALF // TC, step, 0)

    def s2(h, what, up):
        i = 0 if up else 1
        low, high = pl.ds(0, TH), pl.ds(TH, TH)
        if what == 0:
            src, dst = pbuf.at[h, FAR, low if up else high], far.at[h, i]
        else:
            rows = (high if up else low) if what == 1 else (low if up else high)
            src, dst = pbuf.at[h, UP if up else DOWN, rows], near.at[h, i, rows]
        return pltpu.make_async_remote_copy(src_ref=src, dst_ref=dst, send_sem=s2_send.at[h, what, i],
                                            recv_sem=s2_recv.at[h, what, i], device_id=along(1 - h, 1 if up else -1),
                                            device_id_type=MESH_ID)

    for h in range(2):
        for key in sent:
            if key[1] == h and key[0] != 'own':
                arrived(*key)
        combine(h, FAR)
        s2(h, 0, True).start()
        s2(h, 0, False).start()
    for h in range(2):
        combine(h, UP)
        s2(h, 1, True).start()
        combine(h, DOWN)
        s2(h, 1, False).start()
    for h in range(2):
        s2(h, 0, True).wait_recv()
        pbuf[h, UP, 0:TH] += far[h, 0]
        s2(h, 0, False).wait_recv()
        pbuf[h, DOWN, TH:TN] += far[h, 1]
        s2(h, 2, True).start()
        s2(h, 2, False).start()
    for h in range(2):
        for key in sent:
            if key[1] == h and key[0] == 'own':
                arrived(*key)
        combine(h, OWN)
    for h in range(2):
        s2(h, 1, True).wait_recv()
        pbuf[h, OWN, TH:TN] += near[h, 0, TH:TN]
        s2(h, 1, False).wait_recv()
        pbuf[h, OWN, 0:TH] += near[h, 1, 0:TH]
    for h in range(2):
        s2(h, 2, True).wait_recv()
        o_ref[0:TH, h * HALF:(h + 1) * HALF] = (pbuf[h, OWN, 0:TH] + near[h, 0, 0:TH]).astype(o_ref.dtype)
        s2(h, 2, False).wait_recv()
        o_ref[TH:TN, h * HALF:(h + 1) * HALF] = (pbuf[h, OWN, TH:TN] + near[h, 1, TH:TN]).astype(o_ref.dtype)

    for h in range(2):
        for q in range(RING - 1):
            for cp in routes(h, q):
                cp.wait_send()
        for what in range(3):
            for up in (True, False):
                s2(h, what, up).wait_send()
    for key in sent:
        for d, dc in ORDER:
            if (d, dc) != (0, 0):
                s1(*key, d, dc).wait_send()


def solution(mesh):
    token_spec = P(('dp',) + GROUP_AXES, None)
    weight_spec = P(GROUP_AXES, None, None)
    rows_spec = P('dp', GROUP_AXES, None, None)
    YN, XN, CN = (mesh.shape[a] for a in GROUP_AXES)

    def local_part(x_local, w_gate, w_up, w_down, slot_idx, expert_idx, gate_wt):
        _, EN, SN, DN = x_local.shape
        FN = w_gate.shape[2]
        TN, TOP = slot_idx.shape
        HALF = DN // 2
        RING = YN
        KROW = XN * CN * EN * SN
        sizes = (YN, XN, CN, EN, SN, DN, FN, TN)
        bf, f32, i32 = jnp.bfloat16, jnp.float32, jnp.int32
        vm, dma = pltpu.VMEM, pltpu.SemaphoreType.DMA
        any_spec = pl.BlockSpec(memory_space=pltpu.HBM)
        vmem_spec = pl.BlockSpec(memory_space=pltpu.VMEM)
        return pl.pallas_call(
            functools.partial(_body, sizes),
            out_shape=vm((TN, DN), bf),
            in_specs=[any_spec] * 4 + [vmem_spec] * 3,
            out_specs=vmem_spec,
            scratch_shapes=[
                vm((2, YN * XN * CN, SN, DN), bf), vm((2, DN, FN), bf), vm((2, DN, FN), bf), vm((2, FN, DN), bf),
                vm((YN * XN * CN * SN, FN), bf),
                vm((EN, YN, XN, CN, SN, HALF), bf), vm((EN, XN, YN, CN, SN, HALF), bf),
                vm((2, RING, RING, CN, EN, SN, HALF), bf),
                vm((2, RING, 3 * TN, KROW), bf),
                vm((2, RING, TN, HALF), f32),
                vm((2, 2, TN // 2, HALF), f32),
                vm((2, 2, TN, HALF), f32),
                vm((2, RING, TOP, TN), i32), vm((2, RING, TOP, TN), i32), vm((2, RING, TOP, TN), f32),
                dma((2, RING)), dma((2, FN // min(256, FN))), dma((2, FN // min(256, FN))), dma((2,)),
                dma((2, RING, 3)), dma((2, RING, 3)), dma((2 * EN + 4,)),
                dma((2 * EN + 4, RING, CN)), dma((2 * EN + 4, RING, CN)), dma((2, 3, 2)), dma((2, 3, 2)),
            ],
            compiler_params=pltpu.CompilerParams(collective_id=0, has_side_effects=True,
                                                 vmem_limit_bytes=62 * 2 ** 20),
        )(x_local, w_gate, w_up, w_down, slot_idx.T, expert_idx.T, gate_wt.T)

    return jax.shard_map(local_part, mesh=mesh,
                         in_specs=(rows_spec, weight_spec, weight_spec, weight_spec, token_spec, token_spec, token_spec),
                         out_specs=token_spec, check_vma=False)
```

```python
import functools

import jax
import jax.numpy as jnp
from jax import lax
from jax.experimental import pallas as pl
from jax.experimental.pallas import tpu as pltpu
from jax.sharding import PartitionSpec as P

GROUP_AXES = ('eo', 'em', 'ei')
MESH_ID = pl.DeviceIdType.MESH
BF16_MAX = 3.3895313892515355e38


def _split3(w):
    hi = w.astype(jnp.bfloat16)
    rest = w - hi.astype(jnp.float32)
    mid = rest.astype(jnp.bfloat16)
    low = (rest - mid.astype(jnp.float32)).astype(jnp.bfloat16)
    return jnp.concatenate([hi, mid, low], axis=0)


def _body(sizes, x_hbm, wg_hbm, wu_hbm, wd_hbm, slot_hbm, exp_hbm, gate_hbm, o_ref,
          xbuf, wgbuf, wubuf, wdbuf, hbuf, ya, yb, rbuf, wbuf, pbuf, far, near,
          rslot, rexp, rgate, slot_ref, exp_ref, gate_ref,
          own_sem, x_sem, wg_sem, wu_sem, wd_sem, route_send, route_recv, loc_sem, s1_send, s1_recv, s2_send, s2_recv):
    YN, XN, CN, EN, SN, DN, FN, TN = sizes
    RING = YN
    HALF = DN // 2
    QROWS = XN * CN * SN
    KROW = XN * CN * EN * SN
    TF = min(256, FN)
    TD = min(1024, HALF)
    TC = min(256, HALF)
    TH = TN // 2
    UP, FAR, DOWN, OWN = 0, 1, 2, 3
    y = lax.axis_index('eo')
    x = lax.axis_index('em')
    c = lax.axis_index('ei')

    def at(dy, dx, dc):
        return {'eo': lax.rem(y + dy + YN, YN), 'em': lax.rem(x + dx + XN, XN), 'ei': lax.rem(c + dc + CN, CN)}

    def along(h, d, dc=0):
        return at(d, 0, dc) if h else at(0, d, dc)

    def load_x(e, q):
        ys = lax.rem(y + q + 1, YN)
        return pltpu.make_async_copy(x_hbm.at[pl.ds(ys * XN * CN, XN * CN), e],
                                     xbuf.at[e % 2, pl.ds(q * XN * CN, XN * CN)], x_sem.at[e % 2, q])

    def load_tile(e, src, dst, sem, n):
        cols = pl.ds(pl.multiple_of(n * TF, TF), TF)
        return pltpu.make_async_copy(src.at[e, :, cols], dst.at[e % 2, :, cols], sem.at[e % 2, n])

    def load_down(e):
        return pltpu.make_async_copy(wd_hbm.at[e], wdbuf.at[e % 2], wd_sem.at[e % 2])

    NT = FN // TF

    def start_loads(e):
        for q in range(2):
            load_x(e, q).start()
        for n in range(NT):
            load_tile(e, wg_hbm, wgbuf, wg_sem, n).start()
            load_tile(e, wu_hbm, wubuf, wu_sem, n).start()
        for q in range(2, RING):
            load_x(e, q).start()
        load_down(e).start()

    peers = [at(0, d, dc) for d in range(XN) for dc in range(CN) if (d, dc) != (0, 0)]
    peers += [at(d, 0, dc) for d in range(1, YN) for dc in range(CN)]
    barrier = pltpu.get_barrier_semaphore()
    for p in peers:
        pl.semaphore_signal(barrier, inc=1, device_id=p, device_id_type=MESH_ID)

    start_loads(0)
    own = [pltpu.make_async_copy(src, dst, own_sem.at[i])
           for i, (src, dst) in enumerate(((slot_hbm, slot_ref), (exp_hbm, exp_ref), (gate_hbm, gate_ref)))]
    for cp in own:
        cp.start()

    def routes(h, q):
        dev = along(1 - h, -(q + 1))
        return [pltpu.make_async_remote_copy(src_ref=src, dst_ref=dst.at[h, q], send_sem=route_send.at[h, q, i],
                                             recv_sem=route_recv.at[h, q, i], device_id=dev, device_id_type=MESH_ID)
                for i, (src, dst) in enumerate(((slot_ref, rslot), (exp_ref, rexp), (gate_ref, rgate)))]

    messages = {}

    def s1(name, h, es, qs, d, dc):
        i = messages.setdefault((name, h), len(messages))
        tgt = along(h, d, dc)
        if es[1] - es[0] == 1:
            esl, qsl = es[0], pl.ds(qs[0], qs[1] - qs[0])
        else:
            esl, qsl = pl.ds(es[0], es[1] - es[0]), qs[0]
        if h == 0:
            src = ya.at[esl, qsl, tgt['em'], tgt['ei']]
            dst = rbuf.at[0, qsl, x, c, esl]
        else:
            src = yb.at[esl, qsl, (d + RING - 1) % RING, tgt['ei']]
            dst = rbuf.at[1, qsl, y, c, esl]
        if (d, dc) == (0, 0):
            return pltpu.make_async_copy(src, dst, loc_sem.at[i])
        return pltpu.make_async_remote_copy(src_ref=src, dst_ref=dst, send_sem=s1_send.at[i, d, dc],
                                            recv_sem=s1_recv.at[i, d, dc], device_id=tgt, device_id_type=MESH_ID)

    ORDER = [(2, 0), (1, 0), (3, 0), (2, 1), (1, 1), (3, 1), (0, 1), (0, 0)]
    sent = []

    def send(name, h, es, qs, ds=(0, 1, 2, 3)):
        if (name, h, es, qs) not in sent:
            sent.append((name, h, es, qs))
        for d, dc in ORDER:
            if d in ds:
                s1(name, h, es, qs, d, dc).start()

    def arrived(name, h, es, qs):
        for d, dc in ORDER:
            cp = s1(name, h, es, qs, d, dc)
            cp.wait() if (d, dc) == (0, 0) else cp.wait_recv()

    def gate_up(e, q0, q1, tf, waits):
        b = e % 2
        rows = (q1 - q0) * QROWS
        if waits and tf != TF:
            for n in range(NT):
                load_tile(e, wg_hbm, wgbuf, wg_sem, n).wait()
                load_tile(e, wu_hbm, wubuf, wu_sem, n).wait()

        def step(n, carry):
            cols = pl.ds(pl.multiple_of(n * tf, tf), tf)
            if waits and tf == TF:
                load_tile(e, wg_hbm, wgbuf, wg_sem, n).wait()
                load_tile(e, wu_hbm, wubuf, wu_sem, n).wait()
            xv = xbuf[b, q0 * XN * CN:q1 * XN * CN].reshape(rows, DN)
            g = jnp.dot(xv, wgbuf[b, :, cols], preferred_element_type=jnp.float32)
            u = jnp.dot(xv, wubuf[b, :, cols], preferred_element_type=jnp.float32)
            hbuf[q0 * QROWS:q1 * QROWS, cols] = (jax.nn.silu(g) * u).astype(jnp.bfloat16)
            return carry
        lax.fori_loop(0, FN // tf, step, 0)

    def down(e, q0, q1, h):
        b = e % 2

        def step(n, carry):
            wcols = pl.ds(pl.multiple_of(h * HALF + n * TD, TD), TD)
            cols = pl.ds(pl.multiple_of(n * TD, TD), TD)
            v = jnp.dot(hbuf[q0 * QROWS:q1 * QROWS], wdbuf[b, :, wcols], preferred_element_type=jnp.float32)
            v = jnp.where(jnp.abs(v) < BF16_MAX, v, 0.0)
            v = v.astype(jnp.bfloat16).reshape(q1 - q0, XN, CN, SN, TD)
            if h == 0:
                ya[e, q0:q1, :, :, :, cols] = v
            else:
                for xs in range(XN):
                    yb[e, lax.rem(xs - x - 1 + 2 * XN, XN), q0:q1, :, :, cols] = v[:, xs]
            return carry
        lax.fori_loop(0, HALF // TD, step, 0)

    for q in range(2):
        load_x(0, q).wait()
    gate_up(0, 0, 2, TF, True)
    load_down(0).wait()
    down(0, 0, 2, 0)
    pl.semaphore_wait(barrier, len(peers))
    send('a', 0, (0, 1), (0, 2))
    down(0, 0, 2, 1)
    send('a', 1, (0, 1), (0, 4), (1, 2))
    for cp in own:
        cp.wait()
    for h in range(2):
        for q in range(RING - 1):
            for cp in routes(h, q):
                cp.start()
    for q in range(2, RING):
        load_x(0, q).wait()
    start_loads(1)
    gate_up(0, 2, 4, FN, False)
    down(0, 2, 4, 0)
    send('b', 0, (0, 1), (2, 4))
    down(0, 2, 4, 1)
    send('a', 1, (0, 1), (0, 4), (3, 0))

    HELD = EN - 2
    for e in range(1, EN):
        for q in range(RING):
            load_x(e, q).wait()
        if e + 1 < EN:
            start_loads(e + 1)
        gate_up(e, 0, RING, FN, True)
        load_down(e).wait()
        for h in range(2):
            down(e, 0, RING, h)
            send(e, h, (e, e + 1), (0, RING if e < HELD else RING - 1))
    for h in range(2):
        send('own', h, (HELD, EN), (OWN, OWN + 1))

    def build(h, q):
        if q == OWN:
            sl, ex, ga = slot_ref[...], exp_ref[...], gate_ref[...]
        else:
            sl, ex, ga = rslot[h, q], rexp[h, q], rgate[h, q]
        code = jnp.where(sl >= 0, ex * SN + sl, -1)
        if h == 0:
            col = jnp.where(code >= 0, code - y * KROW, -1)
        else:
            blk = CN * EN * SN
            ye = code // KROW
            rem = code - ye * KROW - x * blk
            col = jnp.where((code >= 0) & (rem >= 0) & (rem < blk), ye * blk + rem, -1)
        col = jnp.transpose(col.astype(jnp.float32)).astype(jnp.int32)
        ga = jnp.transpose(ga)
        lanes = lax.broadcasted_iota(jnp.int32, (TN, KROW), 1)
        w = jnp.zeros((TN, KROW), jnp.float32)
        for j in range(col.shape[1]):
            w = jnp.where(lanes == col[:, j:j + 1], ga[:, j:j + 1], w)
        wbuf[h, q] = _split3(w)

    for h in range(2):
        for q in range(RING):
            if q != OWN:
                for cp in routes(h, q):
                    cp.wait_recv()
            build(h, q)

    def combine(h, q):
        def step(n, carry):
            cols = pl.ds(pl.multiple_of(n * TC, TC), TC)
            rows = rbuf[h, q, :, :, :, :, cols].reshape(KROW, TC)
            v = jnp.dot(wbuf[h, q], rows, preferred_element_type=jnp.float32)
            pbuf[h, q, :, cols] = v[0:TN] + (v[TN:2 * TN] + v[2 * TN:3 * TN])
            return carry
        lax.fori_loop(0, HALF // TC, step, 0)

    def s2(h, what, up):
        i = 0 if up else 1
        low, high = pl.ds(0, TH), pl.ds(TH, TH)
        if what == 0:
            src, dst = pbuf.at[h, FAR, low if up else high], far.at[h, i]
        else:
            rows = (high if up else low) if what == 1 else (low if up else high)
            src, dst = pbuf.at[h, UP if up else DOWN, rows], near.at[h, i, rows]
        return pltpu.make_async_remote_copy(src_ref=src, dst_ref=dst, send_sem=s2_send.at[h, what, i],
                                            recv_sem=s2_recv.at[h, what, i], device_id=along(1 - h, 1 if up else -1),
                                            device_id_type=MESH_ID)

    for h in range(2):
        for key in sent:
            if key[1] == h and key[0] != 'own':
                arrived(*key)
        combine(h, FAR)
        s2(h, 0, True).start()
        s2(h, 0, False).start()
    for h in range(2):
        combine(h, UP)
        s2(h, 1, True).start()
        combine(h, DOWN)
        s2(h, 1, False).start()
    for h in range(2):
        s2(h, 0, True).wait_recv()
        pbuf[h, UP, 0:TH] += far[h, 0]
        s2(h, 0, False).wait_recv()
        pbuf[h, DOWN, TH:TN] += far[h, 1]
        s2(h, 2, True).start()
        s2(h, 2, False).start()
    for h in range(2):
        for key in sent:
            if key[1] == h and key[0] == 'own':
                arrived(*key)
        combine(h, OWN)
    for h in range(2):
        s2(h, 1, True).wait_recv()
        pbuf[h, OWN, TH:TN] += near[h, 0, TH:TN]
        s2(h, 1, False).wait_recv()
        pbuf[h, OWN, 0:TH] += near[h, 1, 0:TH]
    for h in range(2):
        s2(h, 2, True).wait_recv()
        o_ref[0:TH, h * HALF:(h + 1) * HALF] = (pbuf[h, OWN, 0:TH] + near[h, 0, 0:TH]).astype(o_ref.dtype)
        s2(h, 2, False).wait_recv()
        o_ref[TH:TN, h * HALF:(h + 1) * HALF] = (pbuf[h, OWN, TH:TN] + near[h, 1, TH:TN]).astype(o_ref.dtype)

    for h in range(2):
        for q in range(RING - 1):
            for cp in routes(h, q):
                cp.wait_send()
        for what in range(3):
            for up in (True, False):
                s2(h, what, up).wait_send()
    for key in sent:
        for d, dc in ORDER:
            if (d, dc) != (0, 0):
                s1(*key, d, dc).wait_send()


def solution(mesh):
    token_spec = P(('dp',) + GROUP_AXES, None)
    weight_spec = P(GROUP_AXES, None, None)
    rows_spec = P('dp', GROUP_AXES, None, None)
    YN, XN, CN = (mesh.shape[a] for a in GROUP_AXES)

    def local_part(x_local, w_gate, w_up, w_down, slot_idx, expert_idx, gate_wt):
        _, EN, SN, DN = x_local.shape
        FN = w_gate.shape[2]
        TN, TOP = slot_idx.shape
        HALF = DN // 2
        RING = YN
        KROW = XN * CN * EN * SN
        sizes = (YN, XN, CN, EN, SN, DN, FN, TN)
        bf, f32, i32 = jnp.bfloat16, jnp.float32, jnp.int32
        vm, dma = pltpu.VMEM, pltpu.SemaphoreType.DMA
        any_spec = pl.BlockSpec(memory_space=pltpu.HBM)
        vmem_spec = pl.BlockSpec(memory_space=pltpu.VMEM)
        return pl.pallas_call(
            functools.partial(_body, sizes),
            out_shape=vm((TN, DN), bf),
            in_specs=[any_spec] * 7,
            out_specs=vmem_spec,
            scratch_shapes=[
                vm((2, YN * XN * CN, SN, DN), bf), vm((2, DN, FN), bf), vm((2, DN, FN), bf), vm((2, FN, DN), bf),
                vm((YN * XN * CN * SN, FN), bf),
                vm((EN, YN, XN, CN, SN, HALF), bf), vm((EN, XN, YN, CN, SN, HALF), bf),
                vm((2, RING, RING, CN, EN, SN, HALF), bf),
                vm((2, RING, 3 * TN, KROW), bf),
                vm((2, RING, TN, HALF), f32),
                vm((2, 2, TN // 2, HALF), f32),
                vm((2, 2, TN, HALF), f32),
                vm((2, RING, TOP, TN), i32), vm((2, RING, TOP, TN), i32), vm((2, RING, TOP, TN), f32),
                vm((TOP, TN), i32), vm((TOP, TN), i32), vm((TOP, TN), f32), dma((3,)),
                dma((2, RING)), dma((2, FN // min(256, FN))), dma((2, FN // min(256, FN))), dma((2,)),
                dma((2, RING, 3)), dma((2, RING, 3)), dma((2 * EN + 4,)),
                dma((2 * EN + 4, RING, CN)), dma((2 * EN + 4, RING, CN)), dma((2, 3, 2)), dma((2, 3, 2)),
            ],
            compiler_params=pltpu.CompilerParams(collective_id=0, has_side_effects=True,
                                                 vmem_limit_bytes=62 * 2 ** 20),
        )(x_local, w_gate, w_up, w_down, slot_idx.T, expert_idx.T, gate_wt.T)

    return jax.shard_map(local_part, mesh=mesh,
                         in_specs=(rows_spec, weight_spec, weight_spec, weight_spec, token_spec, token_spec, token_spec),
                         out_specs=token_spec, check_vma=False)
```

```python
import functools

import jax
import jax.numpy as jnp
from jax import lax
from jax.experimental import pallas as pl
from jax.experimental.pallas import tpu as pltpu
from jax.sharding import PartitionSpec as P

GROUP_AXES = ('eo', 'em', 'ei')
MESH_ID = pl.DeviceIdType.MESH
BF16_MAX = 3.3895313892515355e38


def _split3(w):
    hi = w.astype(jnp.bfloat16)
    rest = w - hi.astype(jnp.float32)
    mid = rest.astype(jnp.bfloat16)
    low = (rest - mid.astype(jnp.float32)).astype(jnp.bfloat16)
    return jnp.concatenate([hi, mid, low], axis=0)


def _body(sizes, x_hbm, wg_hbm, wu_hbm, wd_hbm, slot_hbm, exp_hbm, gate_hbm, o_ref,
          xbuf, wgbuf, wubuf, wdbuf, hbuf, ya, yb, rbuf, wbuf, pbuf, far, near,
          rslot, rexp, rgate, slot_ref, exp_ref, gate_ref,
          own_sem, x_sem, wg_sem, wu_sem, wd_sem, route_send, route_recv, loc_sem, s1_send, s1_recv, s2_send, s2_recv):
    YN, XN, CN, EN, SN, DN, FN, TN = sizes
    RING = YN
    HALF = DN // 2
    QROWS = XN * CN * SN
    KROW = XN * CN * EN * SN
    TF = min(256, FN)
    TD = min(1024, HALF)
    TC = min(256, HALF)
    TH = TN // 2
    UP, FAR, DOWN, OWN = 0, 1, 2, 3
    y = lax.axis_index('eo')
    x = lax.axis_index('em')
    c = lax.axis_index('ei')

    def at(dy, dx, dc):
        return {'eo': lax.rem(y + dy + YN, YN), 'em': lax.rem(x + dx + XN, XN), 'ei': lax.rem(c + dc + CN, CN)}

    def along(h, d, dc=0):
        return at(d, 0, dc) if h else at(0, d, dc)

    def load_x(e, q):
        ys = lax.rem(y + q + 1, YN)
        return pltpu.make_async_copy(x_hbm.at[pl.ds(ys * XN * CN, XN * CN), e],
                                     xbuf.at[e % 2, pl.ds(q * XN * CN, XN * CN)], x_sem.at[e % 2, q])

    def load_tile(e, src, dst, sem, n):
        cols = pl.ds(pl.multiple_of(n * TF, TF), TF)
        return pltpu.make_async_copy(src.at[e, :, cols], dst.at[e % 2, :, cols], sem.at[e % 2, n])

    def load_down(e):
        return pltpu.make_async_copy(wd_hbm.at[e], wdbuf.at[e % 2], wd_sem.at[e % 2])

    NT = FN // TF

    def start_loads(e):
        for q in range(2):
            load_x(e, q).start()
        for n in range(NT):
            load_tile(e, wg_hbm, wgbuf, wg_sem, n).start()
            load_tile(e, wu_hbm, wubuf, wu_sem, n).start()
        for q in range(2, RING):
            load_x(e, q).start()
        load_down(e).start()

    peers = [at(0, d, dc) for d in range(XN) for dc in range(CN) if (d, dc) != (0, 0)]
    peers += [at(d, 0, dc) for d in range(1, YN) for dc in range(CN)]
    barrier = pltpu.get_barrier_semaphore()
    for p in peers:
        pl.semaphore_signal(barrier, inc=1, device_id=p, device_id_type=MESH_ID)

    start_loads(0)
    own = [pltpu.make_async_copy(src, dst, own_sem.at[i])
           for i, (src, dst) in enumerate(((slot_hbm, slot_ref), (exp_hbm, exp_ref), (gate_hbm, gate_ref)))]
    for cp in own:
        cp.start()

    def routes(h, q):
        dev = along(1 - h, -(q + 1))
        return [pltpu.make_async_remote_copy(src_ref=src, dst_ref=dst.at[h, q], send_sem=route_send.at[h, q, i],
                                             recv_sem=route_recv.at[h, q, i], device_id=dev, device_id_type=MESH_ID)
                for i, (src, dst) in enumerate(((slot_ref, rslot), (exp_ref, rexp), (gate_ref, rgate)))]

    messages = {}

    def s1(name, h, es, qs, d, dc):
        i = messages.setdefault((name, h), len(messages))
        tgt = along(h, d, dc)
        if es[1] - es[0] == 1:
            esl, qsl = es[0], pl.ds(qs[0], qs[1] - qs[0])
        else:
            esl, qsl = pl.ds(es[0], es[1] - es[0]), qs[0]
        if h == 0:
            src = ya.at[esl, qsl, tgt['em'], tgt['ei']]
            dst = rbuf.at[0, qsl, x, c, esl]
        else:
            src = yb.at[esl, qsl, (d + RING - 1) % RING, tgt['ei']]
            dst = rbuf.at[1, qsl, y, c, esl]
        if (d, dc) == (0, 0):
            return pltpu.make_async_copy(src, dst, loc_sem.at[i])
        return pltpu.make_async_remote_copy(src_ref=src, dst_ref=dst, send_sem=s1_send.at[i, d, dc],
                                            recv_sem=s1_recv.at[i, d, dc], device_id=tgt, device_id_type=MESH_ID)

    ORDER = [(2, 1), (1, 1), (3, 1), (2, 0), (1, 0), (3, 0), (0, 1), (0, 0)]
    sent = []

    def send(name, h, es, qs, ds=(0, 1, 2, 3)):
        if (name, h, es, qs) not in sent:
            sent.append((name, h, es, qs))
        for d, dc in ORDER:
            if d in ds:
                s1(name, h, es, qs, d, dc).start()

    def arrived(name, h, es, qs):
        for d, dc in ORDER:
            cp = s1(name, h, es, qs, d, dc)
            cp.wait() if (d, dc) == (0, 0) else cp.wait_recv()

    def gate_up(e, q0, q1, tf, waits):
        b = e % 2
        rows = (q1 - q0) * QROWS
        if waits and tf != TF:
            for n in range(NT):
                load_tile(e, wg_hbm, wgbuf, wg_sem, n).wait()
                load_tile(e, wu_hbm, wubuf, wu_sem, n).wait()

        def step(n, carry):
            cols = pl.ds(pl.multiple_of(n * tf, tf), tf)
            if waits and tf == TF:
                load_tile(e, wg_hbm, wgbuf, wg_sem, n).wait()
                load_tile(e, wu_hbm, wubuf, wu_sem, n).wait()
            xv = xbuf[b, q0 * XN * CN:q1 * XN * CN].reshape(rows, DN)
            g = jnp.dot(xv, wgbuf[b, :, cols], preferred_element_type=jnp.float32)
            u = jnp.dot(xv, wubuf[b, :, cols], preferred_element_type=jnp.float32)
            hbuf[q0 * QROWS:q1 * QROWS, cols] = (jax.nn.silu(g) * u).astype(jnp.bfloat16)
            return carry
        lax.fori_loop(0, FN // tf, step, 0)

    def down(e, q0, q1, h):
        b = e % 2

        def step(n, carry):
            wcols = pl.ds(pl.multiple_of(h * HALF + n * TD, TD), TD)
            cols = pl.ds(pl.multiple_of(n * TD, TD), TD)
            v = jnp.dot(hbuf[q0 * QROWS:q1 * QROWS], wdbuf[b, :, wcols], preferred_element_type=jnp.float32)
            v = jnp.where(jnp.abs(v) < BF16_MAX, v, 0.0)
            v = v.astype(jnp.bfloat16).reshape(q1 - q0, XN, CN, SN, TD)
            if h == 0:
                ya[e, q0:q1, :, :, :, cols] = v
            else:
                for xs in range(XN):
                    yb[e, lax.rem(xs - x - 1 + 2 * XN, XN), q0:q1, :, :, cols] = v[:, xs]
            return carry
        lax.fori_loop(0, HALF // TD, step, 0)

    for q in range(2):
        load_x(0, q).wait()
    gate_up(0, 0, 2, TF, True)
    load_down(0).wait()
    down(0, 0, 2, 0)
    pl.semaphore_wait(barrier, len(peers))
    send('a', 0, (0, 1), (0, 2))
    down(0, 0, 2, 1)
    send('a', 1, (0, 1), (0, 4), (1, 2))
    for cp in own:
        cp.wait()
    for h in range(2):
        for q in range(RING - 1):
            for cp in routes(h, q):
                cp.start()
    for q in range(2, RING):
        load_x(0, q).wait()
    start_loads(1)
    gate_up(0, 2, 4, FN, False)
    down(0, 2, 4, 0)
    send('b', 0, (0, 1), (2, 4))
    down(0, 2, 4, 1)
    send('a', 1, (0, 1), (0, 4), (3, 0))

    HELD = EN - 2
    for e in range(1, EN):
        for q in range(RING):
            load_x(e, q).wait()
        if e + 1 < EN:
            start_loads(e + 1)
        gate_up(e, 0, RING, FN, True)
        load_down(e).wait()
        for h in range(2):
            down(e, 0, RING, h)
            send(e, h, (e, e + 1), (0, RING if e < HELD else RING - 1))
    for h in range(2):
        send('own', h, (HELD, EN), (OWN, OWN + 1))

    def build(h, q):
        if q == OWN:
            sl, ex, ga = slot_ref[...], exp_ref[...], gate_ref[...]
        else:
            sl, ex, ga = rslot[h, q], rexp[h, q], rgate[h, q]
        code = jnp.where(sl >= 0, ex * SN + sl, -1)
        if h == 0:
            col = jnp.where(code >= 0, code - y * KROW, -1)
        else:
            blk = CN * EN * SN
            ye = code // KROW
            rem = code - ye * KROW - x * blk
            col = jnp.where((code >= 0) & (rem >= 0) & (rem < blk), ye * blk + rem, -1)
        col = jnp.transpose(col.astype(jnp.float32)).astype(jnp.int32)
        ga = jnp.transpose(ga)
        lanes = lax.broadcasted_iota(jnp.int32, (TN, KROW), 1)
        w = jnp.zeros((TN, KROW), jnp.float32)
        for j in range(col.shape[1]):
            w = jnp.where(lanes == col[:, j:j + 1], ga[:, j:j + 1], w)
        wbuf[h, q] = _split3(w)

    for h in range(2):
        for q in range(RING):
            if q != OWN:
                for cp in routes(h, q):
                    cp.wait_recv()
            build(h, q)

    def combine(h, q):
        def step(n, carry):
            cols = pl.ds(pl.multiple_of(n * TC, TC), TC)
            rows = rbuf[h, q, :, :, :, :, cols].reshape(KROW, TC)
            v = jnp.dot(wbuf[h, q], rows, preferred_element_type=jnp.float32)
            pbuf[h, q, :, cols] = v[0:TN] + (v[TN:2 * TN] + v[2 * TN:3 * TN])
            return carry
        lax.fori_loop(0, HALF // TC, step, 0)

    def s2(h, what, up):
        i = 0 if up else 1
        low, high = pl.ds(0, TH), pl.ds(TH, TH)
        if what == 0:
            src, dst = pbuf.at[h, FAR, low if up else high], far.at[h, i]
        else:
            rows = (high if up else low) if what == 1 else (low if up else high)
            src, dst = pbuf.at[h, UP if up else DOWN, rows], near.at[h, i, rows]
        return pltpu.make_async_remote_copy(src_ref=src, dst_ref=dst, send_sem=s2_send.at[h, what, i],
                                            recv_sem=s2_recv.at[h, what, i], device_id=along(1 - h, 1 if up else -1),
                                            device_id_type=MESH_ID)

    for h in range(2):
        for key in sent:
            if key[1] == h and key[0] != 'own':
                arrived(*key)
        combine(h, FAR)
        s2(h, 0, True).start()
        s2(h, 0, False).start()
    for h in range(2):
        combine(h, UP)
        s2(h, 1, True).start()
        combine(h, DOWN)
        s2(h, 1, False).start()
    for h in range(2):
        s2(h, 0, True).wait_recv()
        pbuf[h, UP, 0:TH] += far[h, 0]
        s2(h, 0, False).wait_recv()
        pbuf[h, DOWN, TH:TN] += far[h, 1]
        s2(h, 2, True).start()
        s2(h, 2, False).start()
    for h in range(2):
        for key in sent:
            if key[1] == h and key[0] == 'own':
                arrived(*key)
        combine(h, OWN)
    for h in range(2):
        s2(h, 1, True).wait_recv()
        pbuf[h, OWN, TH:TN] += near[h, 0, TH:TN]
        s2(h, 1, False).wait_recv()
        pbuf[h, OWN, 0:TH] += near[h, 1, 0:TH]
    for h in range(2):
        s2(h, 2, True).wait_recv()
        o_ref[0:TH, h * HALF:(h + 1) * HALF] = (pbuf[h, OWN, 0:TH] + near[h, 0, 0:TH]).astype(o_ref.dtype)
        s2(h, 2, False).wait_recv()
        o_ref[TH:TN, h * HALF:(h + 1) * HALF] = (pbuf[h, OWN, TH:TN] + near[h, 1, TH:TN]).astype(o_ref.dtype)

    for h in range(2):
        for q in range(RING - 1):
            for cp in routes(h, q):
                cp.wait_send()
        for what in range(3):
            for up in (True, False):
                s2(h, what, up).wait_send()
    for key in sent:
        for d, dc in ORDER:
            if (d, dc) != (0, 0):
                s1(*key, d, dc).wait_send()


def solution(mesh):
    token_spec = P(('dp',) + GROUP_AXES, None)
    weight_spec = P(GROUP_AXES, None, None)
    rows_spec = P('dp', GROUP_AXES, None, None)
    YN, XN, CN = (mesh.shape[a] for a in GROUP_AXES)

    def local_part(x_local, w_gate, w_up, w_down, slot_idx, expert_idx, gate_wt):
        _, EN, SN, DN = x_local.shape
        FN = w_gate.shape[2]
        TN, TOP = slot_idx.shape
        HALF = DN // 2
        RING = YN
        KROW = XN * CN * EN * SN
        sizes = (YN, XN, CN, EN, SN, DN, FN, TN)
        bf, f32, i32 = jnp.bfloat16, jnp.float32, jnp.int32
        vm, dma = pltpu.VMEM, pltpu.SemaphoreType.DMA
        any_spec = pl.BlockSpec(memory_space=pltpu.HBM)
        vmem_spec = pl.BlockSpec(memory_space=pltpu.VMEM)
        return pl.pallas_call(
            functools.partial(_body, sizes),
            out_shape=vm((TN, DN), bf),
            in_specs=[any_spec] * 7,
            out_specs=vmem_spec,
            scratch_shapes=[
                vm((2, YN * XN * CN, SN, DN), bf), vm((2, DN, FN), bf), vm((2, DN, FN), bf), vm((2, FN, DN), bf),
                vm((YN * XN * CN * SN, FN), bf),
                vm((EN, YN, XN, CN, SN, HALF), bf), vm((EN, XN, YN, CN, SN, HALF), bf),
                vm((2, RING, RING, CN, EN, SN, HALF), bf),
                vm((2, RING, 3 * TN, KROW), bf),
                vm((2, RING, TN, HALF), f32),
                vm((2, 2, TN // 2, HALF), f32),
                vm((2, 2, TN, HALF), f32),
                vm((2, RING, TOP, TN), i32), vm((2, RING, TOP, TN), i32), vm((2, RING, TOP, TN), f32),
                vm((TOP, TN), i32), vm((TOP, TN), i32), vm((TOP, TN), f32), dma((3,)),
                dma((2, RING)), dma((2, FN // min(256, FN))), dma((2, FN // min(256, FN))), dma((2,)),
                dma((2, RING, 3)), dma((2, RING, 3)), dma((2 * EN + 4,)),
                dma((2 * EN + 4, RING, CN)), dma((2 * EN + 4, RING, CN)), dma((2, 3, 2)), dma((2, 3, 2)),
            ],
            compiler_params=pltpu.CompilerParams(collective_id=0, has_side_effects=True,
                                                 vmem_limit_bytes=62 * 2 ** 20),
        )(x_local, w_gate, w_up, w_down, slot_idx.T, expert_idx.T, gate_wt.T)

    return jax.shard_map(local_part, mesh=mesh,
                         in_specs=(rows_spec, weight_spec, weight_spec, weight_spec, token_spec, token_spec, token_spec),
                         out_specs=token_spec, check_vma=False)
```
